32 devices in a mesh: lat: 4 (over y, core), lon: 8 (over z, x).
Axes of the slice: x: 2, y: 2, z: 4, core: 2. Of those that a mesh axis runs over, the one named last changes fastest.
Arguments:
- ensemble: bfloat16 [32, 128, 2048], P('lat', 'lon'), may hold values from -6 to 6
- channel_weights: bfloat16 [4, 8, 32, 32, 128], P('lat', 'lon'), may hold values from -1 to 1
- block_column: int32 [4, 8, 32], P('lat', 'lon'), may hold values from 0 to 127
- innovation: bfloat16 [4, 8, 32, 128], P('lat', 'lon'), may hold values from -6 to 6
- error_precision: bfloat16 [4, 8, 32, 128], P('lat', 'lon'), may hold values from 0.25 to 4
- block_count: int32 [4, 8], P('lat', 'lon'), may hold values from 1 to 32, as said below
- neighbours: int32 [16, 64, 12], P('lat', 'lon'), may hold values from 0 to 287
Outputs:
- analysis: bfloat16 [32, 128, 2048], P('lat', 'lon')
The draws below stay inside these ranges and needn't reach their ends.
Inputs may be any that keep to these rules, and one draw needn't show every extreme that they name: The live blocks of a tile are its first block_count slots; at least one tile fills all 32 slots.
All inputs are finite; a program needn't handle non-finite values.
Results may differ from the reference program's by a relative error of at most 0.0074.
Values may be sent and summed in bfloat16 or wider, within the bound.
No kernel may reach another device: no remote copies, remote signals or barrier semaphores. Data moves between devices by JAX's collectives and lax.ppermute only.
A program may use at most 64 MiB of HBM per device.

```python
import math
import jax
import jax.numpy as jnp
from jax import lax

K = 64
L = 32
OB = 128
CLAT = 8
CLON = 16
NBLK = 32
NNB = 12
NSI = 6
NLAT = 32
NLON = 128
TLAT = 4
TLON = 8
GLAT = 16
GLON = 64
LOC = 12


def draw_block_count(key, part):
    raw_draw = jax.random.randint(key, (TLAT, TLON), 1, NBLK + 1)
    counts = jnp.maximum(1, raw_draw * raw_draw // NBLK)
    chosen = jax.random.randint(jax.random.fold_in(key, 7), (), 0, TLAT * TLON)
    counts = counts.reshape(-1).at[chosen].set(NBLK).reshape(TLAT, TLON)
    return counts.astype(jnp.int32)


def with_ends(drawn, own_key, smallest, top_value):
    longest = drawn.shape.index(max(drawn.shape))
    spots = []
    for shift in (0, 1):
        where = [jax.random.randint(jax.random.fold_in(own_key, axis), (), 0, length) for axis, length in enumerate(drawn.shape)]
        where[longest] = (where[longest] + shift) % drawn.shape[longest]
        spots.append(tuple(where))
    return drawn.at[spots[0]].set(smallest).at[spots[1]].set(top_value)


def levels(key, shape, shards, smallest, largest):
    factor_of, own = 1.0, jax.random.fold_in(key, 6)
    for dim, blocks in shards:
        draws = jnp.exp(jax.random.uniform(jax.random.fold_in(own, dim), (blocks,), jnp.float32, smallest / len(shards), largest / len(shards)))
        factor_of = factor_of * jnp.repeat(draws, shape[dim] // blocks).reshape([-1 if axis == dim else 1 for axis in range(len(shape))])
    return factor_of


def gaussian(stream_key, dims, width, most, cuts=(), held_as=jnp.bfloat16):
    level = levels(stream_key, dims, cuts, -0.22, 0.18) if cuts else 1.0
    values = jax.random.normal(stream_key, dims, jnp.float32) * width * level
    return jnp.minimum(jnp.maximum(values, -most), most).astype(held_as)


def setup_inputs(seed: int = 0) -> dict:
    key_of = jax.random.split(jax.random.key(seed), 8)
    ensemble = gaussian(key_of[0], (NLAT, NLON, L * K), 1.0, 6.0, ((0, 4), (1, 8)))
    channel_weights = gaussian(key_of[1], (TLAT, TLON, NBLK, L, OB), L ** -0.5, 1.0, ((0, 4), (1, 8)))
    block_column = with_ends(jax.random.randint(key_of[2], (TLAT, TLON, NBLK), 0, CLAT * CLON), jax.random.fold_in(key_of[2], 1), 0, (CLAT * CLON) - 1).astype(jnp.int32)
    innovation = gaussian(key_of[3], (TLAT, TLON, NBLK, OB), 1.0, 6.0, ((0, 4), (1, 8)))
    error_precision = jnp.clip(jnp.exp(math.log(4.0) - 2.7725887 * jax.random.uniform(key_of[4], (TLAT, TLON, NBLK, OB), jnp.float32) ** levels(key_of[4], (TLAT, TLON, NBLK, OB), ((0, 4), (1, 8)), -0.2, 0.2)), 0.25, 4.0).astype(jnp.bfloat16)
    block_count = draw_block_count(jax.random.fold_in(key_of[7], 71), 0)
    neighbours = with_ends(jax.random.randint(key_of[6], (GLAT, GLON, NNB), 0, 9 * NBLK), jax.random.fold_in(key_of[6], 1), 0, (9 * NBLK) - 1).astype(jnp.int32)
    return {"ensemble": ensemble, "channel_weights": channel_weights, "block_column": block_column, "innovation": innovation, "error_precision": error_precision, "block_count": block_count, "neighbours": neighbours}


def newton_schulz(gram_matrix, projected):
    members = gram_matrix.shape[-1]
    identity = jnp.eye(members, dtype=jnp.float32)
    frobenius = jnp.sqrt(lax.optimization_barrier(jnp.sum(gram_matrix * gram_matrix, axis=(1, 2))))
    current = gram_matrix / frobenius[:, None, None]
    inverse = jnp.broadcast_to(identity, gram_matrix.shape)
    for turn_index in range(NSI):
        middle = 1.5 * identity - 0.5 * jnp.einsum('pij,pjk->pik', inverse, current, precision=lax.Precision.HIGHEST)
        current = jnp.einsum('pij,pjk->pik', current, middle, precision=lax.Precision.HIGHEST)
        inverse = jnp.einsum('pij,pjk->pik', middle, inverse, precision=lax.Precision.HIGHEST)
    root_scale = jnp.sqrt(frobenius)
    spread_part = inverse * (jnp.sqrt(jnp.float32(members - 1.0)) / root_scale)[:, None, None]
    halfway = jnp.einsum('pij,pj->pi', inverse, projected, precision=lax.Precision.HIGHEST)
    mean_shift = jnp.einsum('pij,pj->pi', inverse, halfway, precision=lax.Precision.HIGHEST) / frobenius[:, None]
    return (spread_part + mean_shift[:, :, None]).astype(jnp.bfloat16)

def reference(ensemble, channel_weights, block_column, innovation, error_precision, block_count, neighbours):
    half_lat = CLAT // 2
    half_lon = CLON // 2
    innovation_wide = innovation.astype(jnp.float32)
    precision_wide = error_precision.astype(jnp.float32)
    tile_lat = jnp.arange(TLAT, dtype=jnp.int32)[:, None, None]
    tile_lon = jnp.arange(TLON, dtype=jnp.int32)[None, :, None]
    glob_lat = tile_lat * CLAT + block_column // CLON
    glob_lon = tile_lon * CLON + block_column % CLON
    picked = ensemble[glob_lat, glob_lon].reshape(TLAT, TLON, NBLK, L, K).astype(jnp.float32)
    average = lax.optimization_barrier(jnp.mean(picked, axis=4, keepdims=True))
    anomaly = (picked - average).astype(jnp.bfloat16)
    blocks = jnp.einsum('abdlk,abdlo->abdko', anomaly.astype(jnp.float32), channel_weights.astype(jnp.float32), precision=lax.Precision.HIGHEST).astype(jnp.bfloat16)

    def coarse_row(row_index):
        tile_row = row_index // half_lat
        local_row = row_index % half_lat
        listed = neighbours[row_index]
        point_lon = jnp.arange(GLON, dtype=jnp.int32)
        tile_col = (point_lon // half_lon)[:, None]
        local_col = (point_lon % half_lon)[:, None]
        offset = listed // NBLK
        slot_index = listed % NBLK
        step_lat = offset // 3 - 1
        step_lon = offset % 3 - 1
        source_lat = tile_row + step_lat
        valid = (source_lat >= 0) & (source_lat < TLAT)
        source_lat = jnp.clip(source_lat, 0, TLAT - 1)
        source_lon = (tile_col + step_lon) % TLON
        column = block_column[source_lat, source_lon, slot_index]
        north_south = step_lat.astype(jnp.float32) * CLAT + (column // CLON).astype(jnp.float32)
        east_west = step_lon.astype(jnp.float32) * CLON + (column % CLON).astype(jnp.float32)
        delta_lat = north_south - 2.0 * local_row.astype(jnp.float32)
        delta_lon = east_west - 2.0 * local_col.astype(jnp.float32)
        taper = jnp.exp(-(delta_lat * delta_lat + delta_lon * delta_lon) / (2.0 * LOC * LOC))
        live_mask = (valid & (slot_index < block_count[source_lat, source_lon])).astype(jnp.float32)
        weighted = precision_wide[source_lat, source_lon, slot_index] * live_mask[:, :, None]
        root_weight = jnp.sqrt(taper[:, :, None] * weighted)
        chosen = blocks[source_lat, source_lon, slot_index]
        scaled = (root_weight[:, :, None, :] * chosen.astype(jnp.float32)).astype(jnp.bfloat16)
        forced = (root_weight * innovation_wide[source_lat, source_lon, slot_index]).astype(jnp.bfloat16)
        scaled_wide = scaled.astype(jnp.float32)
        gram_matrix = jnp.einsum('pjko,pjlo->pkl', scaled_wide, scaled_wide, precision=lax.Precision.HIGHEST) + (K - 1.0) * jnp.eye(K, dtype=jnp.float32)
        projected = jnp.einsum('pjko,pjo->pk', scaled_wide, forced.astype(jnp.float32), precision=lax.Precision.HIGHEST)
        return newton_schulz(gram_matrix, projected)
    coarse = lax.map(coarse_row, jnp.arange(GLAT, dtype=jnp.int32)).reshape(GLAT, GLON, K * K)
    coarse_ext = jnp.concatenate([coarse, coarse[-1:]], 0)
    coarse_ext = jnp.concatenate([coarse_ext, coarse_ext[:, :1]], 1)
    state_rows = ensemble.reshape(GLAT, 2, NLON, L * K)

    def fine_pair(pieces):
        upper, lower, pair_rows = pieces
        top_row = upper.astype(jnp.float32)
        bottom_row = lower.astype(jnp.float32)
        row_pair = jnp.stack([top_row, 0.5 * (top_row + bottom_row)], 0)
        col_even = row_pair[:, :-1]
        col_odd = 0.5 * (row_pair[:, :-1] + row_pair[:, 1:])
        blended = jnp.stack([col_even, col_odd], 2).reshape(2, NLON, K, K).astype(jnp.bfloat16)
        state_full = pair_rows.reshape(2, NLON, L, K).astype(jnp.float32)
        center = lax.optimization_barrier(jnp.mean(state_full, axis=3, keepdims=True))
        spread = (state_full - center).astype(jnp.bfloat16)
        result = center + jnp.einsum('rclk,rckj->rclj', spread.astype(jnp.float32), blended.astype(jnp.float32), precision=lax.Precision.HIGHEST)
        return result.astype(jnp.bfloat16).reshape(2, NLON, L * K)
    output = lax.map(fine_pair, (coarse_ext[:-1], coarse_ext[1:], state_rows))
    return output.reshape(NLAT, NLON, L * K)
```

```python
import functools
import math

import jax
import jax.numpy as jnp
import numpy as np
from jax import lax
from jax.experimental import pallas as pl
from jax.experimental.pallas import tpu as pltpu
from jax.sharding import PartitionSpec as P

NSI = 6
LOC = 12
F32 = jnp.float32
BF16 = jnp.bfloat16
VMEM = pl.BlockSpec(memory_space=pltpu.VMEM)
SMEM = pl.BlockSpec(memory_space=pltpu.SMEM)
ANY = pl.BlockSpec(memory_space=pl.ANY)
NT = (((1,), (1,)), ((), ()))


def ring(axis, step, periodic):
    n = lax.axis_size(axis)
    pairs = [(s, s + step) for s in range(n)]
    if periodic:
        return [(s, t % n) for s, t in pairs]
    return [(s, t) for s, t in pairs if 0 <= t < n]


def lane_iota(shape):
    return lax.broadcasted_iota(jnp.int32, shape, len(shape) - 1)


def row_iota(shape):
    return lax.broadcasted_iota(jnp.int32, shape, len(shape) - 2)


def mm(a, b):
    return jnp.dot(a, b, preferred_element_type=F32)


def split(x):
    hi = x.astype(BF16)
    return hi, (x - hi.astype(F32)).astype(BF16)


def prepare_kernel(dims, col_ref, count_ref, ens_ref, w_ref, inn_ref, prec_ref, colrow_ref,
                   anom_ref, cent_ref, pack_ref, x_ref, wf_ref):
    rows, cols, members, levels, slots, obs = dims
    pieces = levels // 2
    wide = 2 * members
    for r in range(rows):
        for t in range(pieces):
            x = ens_ref[r, :, t * wide:(t + 1) * wide].astype(F32)
            x_ref[pl.ds(r * cols * pieces + t, cols, stride=pieces), :] = x
    same = (row_iota((wide, wide)) < members) == (lane_iota((wide, wide)) < members)
    averaging = jnp.where(same, 1.0 / members, 0.0).astype(BF16)
    step = cols * pieces
    for r in range(rows):
        x = x_ref[r * step:(r + 1) * step, :]
        c = mm(x.astype(BF16), averaging)
        cent_ref[r * step:(r + 1) * step, :] = c
        anom_ref[r * step:(r + 1) * step, :] = (x - c).astype(BF16)
    wf_ref[...] = w_ref[...].astype(F32)
    group = wide // pieces
    empty = jnp.zeros((pieces, obs), BF16)
    for first in range(0, slots, group):
        picked = [
            anom_ref[pl.ds(pl.multiple_of(col_ref[first + b] * pieces, pieces), pieces), :]
            for b in range(group)
        ]
        turned = jnp.concatenate(picked, 0).astype(F32).T.astype(BF16)
        left = jnp.concatenate([turned[:members], turned[members:]], 1)
        for b in range(group):
            right = []
            for half in range(2):
                part = wf_ref[pl.ds((first + b) * levels + half, pieces, stride=2), :].astype(BF16)
                right += [part if other == b else empty for other in range(group)]
            pack_ref[(first + b) * members:(first + b + 1) * members, :] = mm(
                left, jnp.concatenate(right, 0)).astype(BF16)
    base = slots * members
    pack_ref[base:base + slots, :] = inn_ref[...]
    live = row_iota((slots, obs)) < count_ref[0]
    weighted = jnp.where(live, prec_ref[...].astype(F32), 0.0)
    pack_ref[base + slots:base + 2 * slots, :] = weighted.astype(BF16)
    pack_ref[base + 2 * slots:, :] = colrow_ref[...]


def gram_kernel(dims, targets, place, base_ref, inrow_ref, hot_ref, low_ref, own_ref, high_ref,
                out_ref, buf_ref, inn_ref, root_ref, s_ref, sems):
    rows, cols, members, slots, obs, entries, size, points, lines = dims
    wide = 2 * members
    copies = [
        pltpu.make_async_copy(src, buf_ref.at[pl.ds(t * size, size), :], sems.at[t])
        for t, src in enumerate((low_ref, own_ref, high_ref))
    ]
    for c in copies:
        c.start()
    for c in copies:
        c.wait()
    base = slots * members
    lane1 = lane_iota((1, obs))
    where_col = jnp.zeros((1, obs), F32)
    where_u = jnp.zeros((1, obs), F32)
    spans = []
    for t in range(3):
        inn_ref[t * slots:(t + 1) * slots, :] = buf_ref[
            t * size + base:t * size + base + slots, :].astype(F32)
        spans.append(buf_ref[
            t * size + base + slots:t * size + base + 2 * slots, :].astype(F32))
        here = (lane1 >= t * slots) & (lane1 < (t + 1) * slots)
        line = buf_ref[t * size + base + 2 * slots:(t + 1) * size, :].astype(F32)[:1]
        where_col = jnp.where(here, line, where_col)
        where_u = jnp.where(here, t - 1.0, where_u)
    spans.append(jnp.zeros((obs - 3 * slots, obs), F32))
    qhi, qlo = split(jnp.sqrt(jnp.concatenate(spans, 0)))
    right_hi = jnp.concatenate([qhi, qhi], 0)
    col_row = jnp.floor((where_col + 0.5) / cols)
    col_col = where_col - col_row * cols
    dlat = where_u * rows + col_row
    batch = wide // lines
    for k, d in enumerate(targets):
        for first in range(0, points, batch):
            pieces = []
            for p in range(first, first + batch):
                a, c = place[p]
                north = dlat - 2.0 * a
                east = col_col - (d * cols + 2.0 * c)
                taper = jnp.exp((north * north + east * east) * (-1.0 / (4.0 * LOC * LOC)))
                at = (k * points + p) * lines
                pieces.append(hot_ref[at:at + lines, :] * taper)
            shi, slo = split(jnp.concatenate(pieces, 0))
            at = (k * points + first) * lines
            root_ref[at:at + batch * lines, :] = (
                mm(jnp.concatenate([shi, slo], 1), right_hi) + mm(shi, qlo))
    sub = 16
    lane = lane_iota((members, wide))
    first_half = lane < members
    rr = row_iota((members, wide))
    cc = jnp.where(first_half, lane, lane - members)
    line_half = lane_iota((1, wide)) < members

    def fill(q, buffer):
        for pair in range(2):
            for n in range(entries):
                over = slice(n * obs, (n + 1) * obs)
                extras = []
                for m in range(2):
                    point = q * 4 + pair * 2 + m
                    root = root_ref[pl.ds(point * lines + n, 1), :]
                    at = pl.multiple_of(base_ref[point * entries + n], sub)
                    block = buf_ref[pl.ds(at, members), :].astype(F32)
                    s_ref[buffer, pair, m * members:(m + 1) * members, over] = (
                        block * root).astype(BF16)
                    extra = inn_ref[pl.ds(inrow_ref[point * entries + n], 1), :] * root
                    extras.append(jnp.broadcast_to(extra, (sub // 2, obs)))
                s_ref[buffer, pair, wide:, over] = jnp.concatenate(extras, 0).astype(BF16)

    def finish(q, buffer):
        found = [
            lax.dot_general(s_ref[buffer, pair], s_ref[buffer, pair, :wide], NT,
                            preferred_element_type=F32)
            for pair in range(2)
        ]
        x, y = [jnp.where(first_half, f[:members], f[members:wide]) for f in found]
        px, py = [
            jnp.where(line_half, f[wide:wide + 1], f[wide + sub // 2:wide + sub // 2 + 1])
            for f in found
        ]
        out_ref[q, :members, :] = jnp.where(rr <= cc, x, y)
        dy = jnp.sum(jnp.where(rr == cc, y, 0.0), axis=0, keepdims=True)
        out_ref[q, members:, :] = jnp.concatenate(
            [dy, px, py, jnp.zeros((5, wide), F32)], 0)

    quads = len(targets) * points // 4
    fill(0, 0)

    def two(i, carry):
        fill(2 * i + 1, 1)
        finish(2 * i, 0)
        fill(jnp.minimum(2 * i + 2, quads - 1), 0)
        finish(2 * i + 1, 1)
        return carry

    lax.fori_loop(0, quads // 2, two, 0)


def newton_kernel(members, left_ref, own_ref, right_ref, out_ref,
                  g_ref, pr_ref, sq_ref, z_ref, m_ref,
                  yh_ref, yl_ref, zh_ref, zl_ref, mh_ref, ml_ref):
    quads = own_ref.shape[0]
    wide = 2 * members
    lane = lane_iota((members, wide))
    first_half = lane < members
    rr = row_iota((members, wide))
    cc = jnp.where(first_half, lane, lane - members)
    eye = jnp.where(rr == cc, 1.0, 0.0)
    keep_lo = jnp.where(first_half, 1.0, 0.0).astype(BF16)
    keep_hi = jnp.where(first_half, 0.0, 1.0).astype(BF16)

    def bd(x):
        return jnp.concatenate([x * keep_lo, x * keep_hi], 0)

    def mm3(left, right):
        lhi, llo = left
        rhi, rlo = right
        return mm(jnp.concatenate([lhi, llo], 1), jnp.concatenate([rhi, rhi], 0)) + mm(lhi, rlo)

    for q in range(quads):
        total = left_ref[q] + own_ref[q] + right_ref[q]
        packed = total[:members]
        t = packed.T
        turned = jnp.concatenate([t[:members], t[members:]], 1)
        dy = total[members:members + 1]
        x = jnp.where(rr <= cc, packed, turned)
        y = jnp.where(rr > cc, packed, jnp.where(rr == cc, dy, turned))
        for k, z in enumerate((x, y)):
            z = z + (members - 1.0) * eye
            g_ref[2 * q + k] = z
            sq_ref[2 * q + k:2 * q + k + 1, :] = jnp.sum(z * z, axis=0, keepdims=True)
            pr_ref[2 * q + k:2 * q + k + 1, :] = total[members + 1 + k:members + 2 + k]
    same = (row_iota((wide, wide)) < members) == (lane_iota((wide, wide)) < members)
    ones = jnp.where(same, 1.0, 0.0).astype(BF16)
    sq = sq_ref[...]
    s1 = sq.astype(BF16)
    rest = sq - s1.astype(F32)
    s2, s3 = split(rest)
    frob = jnp.sqrt(mm(s1, ones) + mm(s2, ones) + mm(s3, ones))
    sq_ref[...] = frob

    pairs = range(2 * quads)

    def put(refs, k, value):
        for ref, part in zip(refs, split(value)):
            ref[k] = part

    def bds(refs, k):
        return tuple(bd(ref[k]) for ref in refs)

    def get(refs, k):
        return tuple(ref[k] for ref in refs)

    ys, zs, ms = (yh_ref, yl_ref), (zh_ref, zl_ref), (mh_ref, ml_ref)
    for k in pairs:
        a = g_ref[k] / sq_ref[k:k + 1, :]
        put(zs, k, 1.5 * eye - 0.5 * a)
        put(ys, k, a)
    for k in pairs:
        put(ys, k, mm3(get(zs, k), bds(ys, k)))
    for turn in range(1, NSI):
        for k in pairs:
            put(ms, k, 1.5 * eye - 0.5 * mm3(get(zs, k), bds(ys, k)))
        for k in pairs:
            if turn < NSI - 1:
                yb, zb = bds(ys, k), bds(zs, k)
                both = mm3(get(ms, k), tuple(jnp.concatenate([u, v], 1) for u, v in zip(yb, zb)))
                put(ys, k, both[:, :wide])
                put(zs, k, both[:, wide:])
            else:
                z = mm3(get(ms, k), bds(zs, k))
                z_ref[k] = z
                put(zs, k, z)
    for k in pairs:
        proj = jnp.broadcast_to(pr_ref[k:k + 1, :], (16, wide))
        m_ref[k:k + 1, :] = mm3(split(proj), bds(zs, k))[:1]
    for k in pairs:
        half = jnp.broadcast_to(m_ref[k:k + 1, :], (16, wide))
        pr_ref[k:k + 1, :] = mm3(split(half), bds(zs, k))[:1]
    frob = sq_ref[...]
    shift = (pr_ref[...] / frob).T
    scale = math.sqrt(members - 1.0) / jnp.sqrt(frob)
    for at in range(2 * quads):
        col = jnp.where(first_half, shift[:members, at:at + 1], shift[members:, at:at + 1])
        out_ref[at] = (z_ref[at] * scale[at:at + 1] + col).astype(BF16)


def analysis_kernel(dims, spot, last_ref, own_ref, below_ref, beside_ref, corner_ref, anom_ref,
                    cent_ref, out_ref, d_ref, y_ref):
    rows, cols, members, levels, glat, glon = dims
    wide = 2 * members
    pieces = levels // 2
    lane = lane_iota((members, wide))
    first_half = lane < members
    keep_lo = jnp.where(first_half, 1.0, 0.0).astype(BF16)
    keep_hi = jnp.where(first_half, 0.0, 1.0).astype(BF16)
    ending = last_ref[0] == 1

    def both(pair, half):
        x = pair.astype(F32)
        other = pltpu.roll(x, members, 1)
        return jnp.where(first_half == (half == 0), x, other)

    def own(g, h):
        pair, half = spot[(g, h)]
        return both(own_ref[pair], half)

    def beside(g):
        pair, half = spot[(g, 0)]
        index = 0 if g == 0 else pair - glon // 2 + 1
        return both(beside_ref[index], half)

    for g in range(glat):
        for h in range(glon):
            d_ref[g * (glon + 1) + h] = own(g, h)
        d_ref[g * (glon + 1) + glon] = beside(g)
    for h in range(glon):
        d_ref[glat * (glon + 1) + h] = jnp.where(
            ending, own(glat - 1, h), both(below_ref[h // 2], h % 2))
    d_ref[glat * (glon + 1) + glon] = jnp.where(
        ending, beside(glat - 1), both(corner_ref[0], 0))

    def pair_of_rows(g, carry):
        for odd in range(2):
            r = 2 * g + odd
            line = []
            for h in range(glon + 1):
                t = d_ref[g * (glon + 1) + h]
                if odd:
                    t = 0.5 * (t + d_ref[(g + 1) * (glon + 1) + h])
                line.append(t)
            for c in range(cols):
                b = line[c // 2]
                if c % 2:
                    b = 0.5 * (b + line[c // 2 + 1])
                b = b.astype(BF16)
                b = jnp.concatenate([b * keep_lo, b * keep_hi], 0)
                at = pl.multiple_of((r * cols + c) * pieces, pieces)
                y_ref[c * pieces:(c + 1) * pieces, :] = (
                    cent_ref[pl.ds(at, pieces), :] + mm(anom_ref[pl.ds(at, pieces), :], b))
            for t in range(pieces):
                out_ref[r, :, t * wide:(t + 1) * wide] = y_ref[
                    pl.ds(t, cols, stride=pieces), :].astype(BF16)
        return carry

    lax.fori_loop(0, glat, pair_of_rows, 0)


def body(
    ensemble, channel_weights, block_column, innovation, error_precision, block_count, neighbours
):
    rows, cols, row_width = ensemble.shape
    slots = block_column.shape[2]
    levels, obs = channel_weights.shape[3:]
    members = row_width // levels
    glat, glon, entries = neighbours.shape
    points = glat * glon
    wide = 2 * members
    pieces = levels // 2
    lines = 16
    size = slots * members + 2 * slots + 16
    order = [(0, h) for h in range(glon)] + [(g, 0) for g in range(1, glat)]
    order += [(g, h) for g in range(1, glat) for h in range(1, glon)]
    spot = {p: (i // 2, i % 2) for i, p in enumerate(order)}
    index = np.array([g * glon + h for g, h in order])

    columns = block_column[0, 0]
    colrow = jnp.broadcast_to(
        jnp.tile(columns.astype(BF16), obs // slots)[None], (16, obs))
    nb = neighbours.reshape(points * entries)
    ahead = lax.ppermute(nb, "lon", ring("lon", -1, True))
    behind = lax.ppermute(nb, "lon", ring("lon", 1, True))

    anom, cent, pack = pl.pallas_call(
        functools.partial(prepare_kernel, (rows, cols, members, levels, slots, obs)),
        out_shape=(
            jax.ShapeDtypeStruct((rows * cols * pieces, wide), BF16),
            jax.ShapeDtypeStruct((rows * cols * pieces, wide), F32),
            jax.ShapeDtypeStruct((size, obs), BF16),
        ),
        in_specs=[SMEM, SMEM, VMEM, VMEM, VMEM, VMEM, VMEM],
        out_specs=(VMEM, VMEM, VMEM),
        scratch_shapes=[
            pltpu.VMEM((rows * cols * pieces, wide), F32),
            pltpu.VMEM((slots * levels, obs), F32),
        ],
        compiler_params=pltpu.CompilerParams(vmem_limit_bytes=16 << 20),
        name="prepare",
    )(columns, block_count[0], ensemble, channel_weights.reshape(slots * levels, obs),
      innovation[0, 0], error_precision[0, 0], colrow)

    low = lax.ppermute(pack, "lat", ring("lat", 1, False))
    high = lax.ppermute(pack, "lat", ring("lat", -1, False))

    lists = jnp.stack([ahead, behind, nb]).reshape(3, points, entries)[:, index]
    offset = lists // slots
    wanted = jnp.array([-1, 1, 0], jnp.int32)[:, None, None]
    match = offset % 3 - 1 == wanted
    slot = jnp.where(match, offset // 3 * slots + lists % slots, 0)
    starts = (slot // slots) * size + (slot % slots) * members
    padded = jnp.pad(jnp.where(match, slot, -1), ((0, 0), (0, 0), (0, lines - entries)),
                     constant_values=-1)
    hot = (padded.reshape(3, points * lines, 1) == jnp.arange(obs)).astype(F32)

    def gram(targets, which):
        n = len(targets)
        return pl.pallas_call(
            functools.partial(
                gram_kernel,
                (rows, cols, members, slots, obs, entries, size, points, lines), targets, order),
            out_shape=jax.ShapeDtypeStruct((n * points // 4, members + 8, wide), F32),
            in_specs=[SMEM, SMEM, VMEM, ANY, ANY, ANY],
            out_specs=VMEM,
            scratch_shapes=[
                pltpu.VMEM((3 * size, obs), BF16),
                pltpu.VMEM((3 * slots, obs), F32),
                pltpu.VMEM((n * points * lines, obs), F32),
                pltpu.VMEM((2, 2, wide + 16, entries * obs), BF16),
                pltpu.SemaphoreType.DMA((3,)),
            ],
            compiler_params=pltpu.CompilerParams(vmem_limit_bytes=16 << 20),
            cost_estimate=pl.CostEstimate(
                flops=n * points * 2 * (wide + 16) * wide * entries * obs // 2,
                bytes_accessed=3 * size * obs * 2, transcendentals=0),
            name="gram",
        )(starts[which].reshape(-1), slot[which].reshape(-1), hot[which].reshape(-1, obs),
          low, pack, high)

    sides = gram((1.0, -1.0), slice(0, 2))
    quads = points // 4
    from_left = lax.ppermute(sides[:quads], "lon", ring("lon", 1, True))
    from_right = lax.ppermute(sides[quads:], "lon", ring("lon", -1, True))
    middle = gram((0.0,), slice(2, 3))

    trans = pl.pallas_call(
        functools.partial(newton_kernel, members),
        out_shape=jax.ShapeDtypeStruct((points // 2, members, wide), BF16),
        in_specs=[VMEM, VMEM, VMEM],
        out_specs=VMEM,
        scratch_shapes=[
            pltpu.VMEM((points // 2, members, wide), F32),
            pltpu.VMEM((points // 2, wide), F32),
            pltpu.VMEM((points // 2, wide), F32),
            pltpu.VMEM((points // 2, members, wide), F32),
            pltpu.VMEM((points // 2, wide), F32),
        ] + [pltpu.VMEM((points // 2, members, wide), BF16)] * 6,
        compiler_params=pltpu.CompilerParams(vmem_limit_bytes=16 << 20),
        name="newton",
    )(from_left, middle, from_right)

    below = lax.ppermute(trans[:glon // 2], "lat", ring("lat", -1, False))
    edge = glat // 2
    mine = jnp.concatenate([trans[:1], trans[glon // 2:glon // 2 + edge]], 0)
    beside = lax.ppermute(mine, "lon", ring("lon", -1, True))
    corner = lax.ppermute(below[:1], "lon", ring("lon", -1, True))
    last = (lax.axis_index("lat") == lax.axis_size("lat") - 1).astype(jnp.int32)[None]
    return pl.pallas_call(
        functools.partial(
            analysis_kernel, (rows, cols, members, levels, glat, glon), spot),
        out_shape=jax.ShapeDtypeStruct((rows, cols, row_width), BF16),
        in_specs=[SMEM] + [VMEM] * 6,
        out_specs=VMEM,
        scratch_shapes=[
            pltpu.VMEM(((glat + 1) * (glon + 1), members, wide), F32),
            pltpu.VMEM((cols * pieces, wide), F32),
        ],
        compiler_params=pltpu.CompilerParams(vmem_limit_bytes=16 << 20),
        name="analysis",
    )(last, trans, below, beside, corner, anom, cent)


def solution(mesh):
    return jax.shard_map(
        body,
        mesh=mesh,
        in_specs=(
            P("lat", "lon", None),
            P("lat", "lon", None, None, None),
            P("lat", "lon", None),
            P("lat", "lon", None, None),
            P("lat", "lon", None, None),
            P("lat", "lon"),
            P("lat", "lon", None),
        ),
        out_specs=P("lat", "lon", None),
        check_vma=False,
    )
```
